32 devices in a mesh: seq: 16 (over z, x, core), row: 2 (over y).
Axes of the slice: x: 2, y: 2, z: 4, core: 2. Of those that a mesh axis runs over, the one named last changes fastest.
Arguments:
- patch_queries: bfloat16 [2048, 2048], P('seq', 'row'), may hold values from -15 to 15
- patch_keys: bfloat16 [2048, 2048], P('seq', 'row'), may hold values from -15 to 15
- patch_values: bfloat16 [2048, 2048], P('seq', 'row'), may hold values from -6 to 6
- patch_tasks: int32 [2048], P('seq'), may hold values from 0 to 7
- residual: bfloat16 [2048, 2048], P('seq', 'row'), may hold values from -6 to 6
- output_weight: bfloat16 [2048, 2048], P('row'), may hold values from -0.5 to 0.5
- global_down: bfloat16 [2048, 16], P('row'), may hold values from -0.5 to 0.5
- global_up: bfloat16 [16, 2048], P(None, 'row'), may hold values from -1.5 to 1.5
- global_scales: float32 [8, 16], replicated, may hold values from 0.25 to 4
- local_weight: bfloat16 [2048, 512], P('row'), may hold values from -0.125 to 0.125
- byte_ids: int32 [16384], P('seq'), may hold values from 0 to 255
- byte_table: bfloat16 [256, 512], replicated, may hold values from -6 to 6
- position_table: bfloat16 [8, 512], replicated, may hold values from -6 to 6
- norm_gain: float32 [512], replicated, may hold values from 0.5 to 1.5
- hidden_in: bfloat16 [2048, 512], P('row', 'seq'), may hold values from -0.25 to 0.25
- hidden_out: bfloat16 [2048, 512], P('row', 'seq'), may hold values from -0.125 to 0.125
- local_down: bfloat16 [512, 16], replicated, may hold values from -0.25 to 0.25
- local_up: bfloat16 [16, 2048], P(None, 'row'), may hold values from -1.5 to 1.5
- local_scales: float32 [8, 16], replicated, may hold values from 0.25 to 4
- cotangent: bfloat16 [16384, 512], P(('seq', 'row')), may hold values from -6 to 6
Outputs:
- grad_global_down: float32 [2048, 16], P('row')
- grad_global_up: float32 [16, 2048], P(None, 'row')
- grad_global_scales: float32 [8, 16], replicated
- grad_local_down: float32 [512, 16], replicated
- grad_local_up: float32 [16, 2048], P(None, 'row')
- grad_local_scales: float32 [8, 16], replicated
The draws below stay inside these ranges and needn't reach their ends.
All inputs are finite; a program needn't handle non-finite values.
Results may differ from the reference program's by a relative error of at most 0.028.
Values may be sent and summed in bfloat16 or wider, within the bound.
A program may use at most 64 MiB of HBM per device.

```python
import math
import jax
import jax.numpy as jnp
import numpy as np
from jax import lax

D = 2048
HEADS = 16
HEAD = 128
L = 512
FF_L = 2048
VOCAB = 256
PATCH = 8
RANK = 16
TASKS = 8
PATCHES = 2048
BYTES = 16384
N_ROW = 2


def draw_patch_queries(key, part):
    values = 2.5 * jnp.clip(jax.random.normal(jax.random.fold_in(key, 11), (PATCHES, HEADS * HEAD), jnp.float32), -6.0, 6.0)
    return values.astype(jnp.bfloat16)


def draw_patch_keys(key, part):
    values = jnp.clip(jax.random.normal(jax.random.fold_in(key, 13), (PATCHES, HEADS * HEAD), jnp.float32), -6.0, 6.0)
    return values.astype(jnp.bfloat16)


def plant(array, rng, least, high):
    longest = array.shape.index(max(array.shape))
    spots = []
    for shift in (0, 1):
        where = [jax.random.randint(jax.random.fold_in(rng, axis), (), 0, length) for axis, length in enumerate(array.shape)]
        where[longest] = (where[longest] + shift) % array.shape[longest]
        spots.append(tuple(where))
    return array.at[spots[0]].set(least).at[spots[1]].set(high)


def block_scale(own_key, shape, pieces, smallest, largest):
    loudness = 1.0
    for axis_at, blocks in pieces:
        draws = jax.random.uniform(jax.random.fold_in(jax.random.fold_in(own_key, 6), axis_at), (blocks,), jnp.float32, smallest / len(pieces), largest / len(pieces))
        loudness = loudness * jnp.repeat(jnp.exp(draws), shape[axis_at] // blocks).reshape((-1,) + (1,) * (len(shape) - 1 - axis_at))
    return loudness


def rank_table(count, skew):
    portions = [(1 << 20) // math.isqrt(rank ** skew) + 1 for rank in range(1, count + 1)]
    scale = 1 + sum(portions) // (1 << 30)
    return np.cumsum(np.array([max(1, weight // scale) for weight in portions]))


def skewed_ids(stream_key, dims, count, lean):
    table = rank_table(count, lean)
    lot = jax.random.randint(jax.random.fold_in(stream_key, 1), dims, 0, int(table[count - 1]))
    grade = jnp.searchsorted(jnp.asarray(table, jnp.int32), lot, side="right")
    return jax.random.permutation(jax.random.fold_in(stream_key, 2), count)[grade].astype(jnp.int32)


def centred(own_key, shape, spread, bound, pieces=(), held_as=jnp.bfloat16):
    loudness = block_scale(own_key, shape, pieces, -0.22, 0.18) if pieces else 1.0
    result = jax.random.normal(own_key, shape, jnp.float32) * spread * loudness
    return jnp.minimum(jnp.maximum(result, -bound), bound).astype(held_as)


def setup_inputs(seed: int = 0) -> dict:
    seeds = jax.random.split(jax.random.key(seed), 21)
    patch_queries = draw_patch_queries(jax.random.fold_in(seeds[20], 71), 0)
    patch_keys = draw_patch_keys(jax.random.fold_in(seeds[20], 71), 0)
    patch_values = centred(seeds[2], (PATCHES, HEADS * HEAD), 1.0, 6.0, ((0, 16), (1, 2)))
    patch_tasks = plant(jax.random.randint(seeds[3], (PATCHES,), 0, TASKS), jax.random.fold_in(seeds[3], 1), 0, TASKS - 1).astype(jnp.int32)
    residual = centred(seeds[4], (PATCHES, D), 1.0, 6.0, ((0, 16), (1, 2)))
    output_weight = centred(seeds[5], (HEADS * HEAD, D), HEAD ** -0.5, 0.5, ((0, 2),))
    global_down = centred(seeds[6], (HEADS * HEAD, RANK), HEAD ** -0.5, 0.5, ((0, 2),))
    global_up = centred(seeds[7], (RANK, D), RANK ** -0.5, 1.5, ((1, 2),))
    global_scales = jnp.clip(jnp.exp(jax.random.uniform(seeds[8], (TASKS, RANK), jnp.float32, math.log(0.25), math.log(4.0))), 0.25, 4.0)
    local_weight = centred(seeds[9], (D, L), D ** -0.5, 0.125, ((0, 2),))
    byte_ids = plant(skewed_ids(seeds[10], (BYTES,), VOCAB, 2), jax.random.fold_in(seeds[10], 3), 0, VOCAB - 1).astype(jnp.int32)
    byte_table = centred(seeds[11], (VOCAB, L), 1.0, 6.0)
    position_table = centred(seeds[12], (PATCH, L), 1.0, 6.0)
    norm_gain = jnp.clip(1.0 + 0.1 * jax.random.normal(seeds[13], (L,), jnp.float32), 0.5, 1.5)
    hidden_in = centred(seeds[14], (FF_L, L), L ** -0.5, 0.25, ((0, 2), (1, 16)))
    hidden_out = centred(seeds[15], (FF_L, L), FF_L ** -0.5, 0.125, ((0, 2), (1, 16)))
    local_down = centred(seeds[16], (L, RANK), L ** -0.5, 0.25)
    local_up = centred(seeds[17], (RANK, FF_L), RANK ** -0.5, 1.5, ((1, 2),))
    local_scales = jnp.clip(jnp.exp(jax.random.uniform(seeds[18], (TASKS, RANK), jnp.float32, math.log(0.25), math.log(4.0))), 0.25, 4.0)
    cotangent = centred(seeds[19], (BYTES, L), 1.0, 6.0, ((0, 32),))
    return {"patch_queries": patch_queries, "patch_keys": patch_keys, "patch_values": patch_values, "patch_tasks": patch_tasks, "residual": residual, "output_weight": output_weight, "global_down": global_down, "global_up": global_up, "global_scales": global_scales, "local_weight": local_weight, "byte_ids": byte_ids, "byte_table": byte_table, "position_table": position_table, "norm_gain": norm_gain, "hidden_in": hidden_in, "hidden_out": hidden_out, "local_down": local_down, "local_up": local_up, "local_scales": local_scales, "cotangent": cotangent}


def rounded(value):
    return lax.optimization_barrier(value.astype(jnp.bfloat16)).astype(jnp.float32)

def contract(left, right, left_dim, right_dim):
    return lax.dot_general(left, right, (((left_dim,), (right_dim,)), ((), ())), preferred_element_type=jnp.float32)

def select_rows(table, tasks):
    picks = (tasks[:, None] == jnp.arange(table.shape[0], dtype=jnp.int32)[None, :]).astype(jnp.float32)
    return jnp.dot(picks, table, precision=lax.Precision.HIGHEST)

def task_totals(tasks, values):
    picks = (tasks[:, None] == jnp.arange(TASKS, dtype=jnp.int32)[None, :]).astype(jnp.float32)
    return lax.dot_general(picks, values, (((0,), (0,)), ((), ())), precision=lax.Precision.HIGHEST)

def gelu_slope(upper):
    cumulative = 0.5 * (1.0 + lax.erf(upper * 0.7071067811865476))
    density = jnp.exp(-0.5 * upper * upper) * 0.3989422804014327
    return cumulative + upper * density

def local_inputs(identities, projected, tasks, byte_table, position_table, norm_gain, local_down, local_scales):
    count = identities.shape[0]
    picks = (identities[:, None] == jnp.arange(VOCAB, dtype=jnp.int32)[None, :]).astype(jnp.bfloat16)
    embedded = jnp.dot(picks, byte_table, preferred_element_type=jnp.float32)
    patches = count // PATCH
    inputs = embedded.reshape(patches, PATCH, -1) + position_table.astype(jnp.float32)[None] + projected.astype(jnp.float32)[:, None, :]
    inputs = inputs.reshape(count, -1)
    inverse = lax.rsqrt(lax.optimization_barrier(jnp.mean(inputs * inputs, axis=1, keepdims=True)) + 1e-06)
    normed = (inputs * inverse * norm_gain).astype(jnp.bfloat16)
    lowered = jnp.dot(normed, local_down, preferred_element_type=jnp.float32)
    byte_tasks = jnp.repeat(tasks, PATCH)
    scales = select_rows(local_scales, byte_tasks)
    shrunk = (lowered * scales).astype(jnp.bfloat16)
    return (inputs, inverse, normed, lowered, scales, shrunk, byte_tasks)

def backward_norm(back_total, inputs, inverse, norm_gain, cotangent):
    gained = back_total * norm_gain
    average = lax.optimization_barrier(jnp.mean(gained * inputs, axis=1, keepdims=True))
    return cotangent.astype(jnp.float32) + inverse * (gained - inputs * inverse * inverse * average)

def causal_attention(patch_queries, patch_keys, patch_values):
    total = patch_queries.shape[0]
    width = patch_queries.shape[1]
    heads = width // HEAD
    block = math.gcd(total, 512)
    key_heads = patch_keys.reshape(total, heads, HEAD).astype(jnp.float32)
    value_heads = patch_values.reshape(total, heads, HEAD).astype(jnp.float32)
    places = jnp.arange(total, dtype=jnp.int32)
    scale = 1.0 / math.sqrt(HEAD)

    def one_block(index):
        first = index * block
        query_heads = lax.dynamic_slice_in_dim(patch_queries, first, block, 0).reshape(block, heads, HEAD).astype(jnp.float32)
        scores = jnp.einsum('qhd,khd->hqk', query_heads, key_heads) * scale
        allowed = places[None, :] <= (first + jnp.arange(block, dtype=jnp.int32))[:, None]
        scores = jnp.where(allowed[None], scores, -1e+30)
        top = lax.optimization_barrier(jnp.max(scores, axis=2, keepdims=True))
        weights = jnp.where(allowed[None], jnp.exp(scores - top), 0.0)
        mass = lax.optimization_barrier(jnp.sum(weights, axis=2))
        mixed = jnp.einsum('hqk,khd->qhd', rounded(weights), value_heads)
        mixed = mixed / jnp.transpose(mass)[:, :, None]
        return mixed.reshape(block, width).astype(jnp.bfloat16)
    blocks = lax.map(one_block, jnp.arange(total // block, dtype=jnp.int32))
    return blocks.reshape(total, width)

def reference(patch_queries, patch_keys, patch_values, patch_tasks, residual, output_weight, global_down, global_up, global_scales, local_weight, byte_ids, byte_table, position_table, norm_gain, hidden_in, hidden_out, local_down, local_up, local_scales, cotangent):
    attended = causal_attention(patch_queries, patch_keys, patch_values)
    reduced = jnp.dot(attended, global_down, preferred_element_type=jnp.float32)
    task_scales = select_rows(global_scales, patch_tasks)
    scaled = (reduced * task_scales).astype(jnp.bfloat16)
    mixed = residual.astype(jnp.float32) + jnp.dot(scaled, global_up, preferred_element_type=jnp.float32)
    group = HEADS * HEAD // N_ROW
    for index in range(N_ROW):
        part = jnp.dot(attended[:, index * group:(index + 1) * group], output_weight[index * group:(index + 1) * group], preferred_element_type=jnp.float32)
        mixed = mixed + rounded(part)
    mixed_b = mixed.astype(jnp.bfloat16)
    projected = jnp.dot(mixed_b, local_weight, preferred_element_type=jnp.float32).astype(jnp.bfloat16)
    inputs, inverse, normed, lowered, scales, shrunk, byte_tasks = local_inputs(byte_ids, projected, patch_tasks, byte_table, position_table, norm_gain, local_down, local_scales)
    hidden = FF_L // N_ROW
    back_norm = jnp.zeros(inputs.shape, jnp.float32)
    back_rank = jnp.zeros(lowered.shape, jnp.float32)
    pieces_up = []
    for index in range(N_ROW):
        rows_in = hidden_in[index * hidden:(index + 1) * hidden]
        rows_out = hidden_out[index * hidden:(index + 1) * hidden]
        columns_up = local_up[:, index * hidden:(index + 1) * hidden]
        upper = contract(normed, rows_in, 1, 1) + jnp.dot(shrunk, columns_up, preferred_element_type=jnp.float32)
        through = contract(cotangent, rows_out, 1, 1)
        grown = (through * gelu_slope(upper)).astype(jnp.bfloat16)
        pieces_up.append(contract(shrunk, grown, 0, 0))
        back_norm = back_norm + rounded(jnp.dot(grown, rows_in, preferred_element_type=jnp.float32))
        back_rank = back_rank + rounded(contract(grown, columns_up, 1, 1))
    grad_local_up = jnp.concatenate(pieces_up, axis=1)
    grad_local_scales = task_totals(byte_tasks, back_rank * lowered)
    moved = (back_rank * scales).astype(jnp.bfloat16)
    grad_local_down = contract(normed, moved, 0, 0)
    back_total = back_norm + contract(moved, local_down, 1, 1)
    back_inputs = backward_norm(back_total, inputs, inverse, norm_gain, cotangent)
    patch_grad = back_inputs.reshape(-1, PATCH, back_inputs.shape[1]).sum(axis=1).astype(jnp.bfloat16)
    back_mixed = contract(patch_grad, local_weight, 1, 1).astype(jnp.bfloat16)
    grad_global_up = contract(scaled, back_mixed, 0, 0)
    back_scaled = contract(back_mixed, global_up, 1, 1)
    grad_global_scales = task_totals(patch_tasks, back_scaled * reduced)
    back_reduced = (back_scaled * task_scales).astype(jnp.bfloat16)
    grad_global_down = contract(attended, back_reduced, 0, 0)
    return (grad_global_down, grad_global_up, grad_global_scales, grad_local_down, grad_local_up, grad_local_scales)
```

```python
import functools
import math

import jax
import jax.numpy as jnp
from jax import lax
from jax.experimental import pallas as pl
from jax.experimental.pallas import tpu as pltpu
from jax.sharding import PartitionSpec as P

HEAD = 128
VOCAB = 256
PATCH = 8
TASKS = 8


def contract(left, right, left_dim, right_dim):
    return lax.dot_general(
        left, right, (((left_dim,), (right_dim,)), ((), ())), preferred_element_type=jnp.float32
    )


def select_rows(table, tasks):
    picks = (tasks[:, None] == jnp.arange(table.shape[0], dtype=jnp.int32)[None, :]).astype(
        jnp.float32
    )
    return jnp.dot(picks, table, precision=lax.Precision.HIGHEST)


def task_totals(tasks, values):
    picks = (tasks[:, None] == jnp.arange(TASKS, dtype=jnp.int32)[None, :]).astype(jnp.float32)
    return lax.dot_general(picks, values, (((0,), (0,)), ((), ())), precision=lax.Precision.HIGHEST)


def gelu_slope(upper):
    cumulative = 0.5 * (1.0 + lax.erf(upper * 0.7071067811865476))
    density = jnp.exp(-0.5 * upper * upper) * 0.3989422804014327
    return cumulative + upper * density


def local_inputs(
    identities, projected, tasks, byte_table, position_table, norm_gain, local_down, local_scales
):
    count = identities.shape[0]
    picks = (identities[:, None] == jnp.arange(VOCAB, dtype=jnp.int32)[None, :]).astype(
        jnp.bfloat16
    )
    embedded = jnp.dot(picks, byte_table, preferred_element_type=jnp.float32)
    patches = count // PATCH
    inputs = (
        embedded.reshape(patches, PATCH, -1)
        + position_table.astype(jnp.float32)[None]
        + projected.astype(jnp.float32)[:, None, :]
    )
    inputs = inputs.reshape(count, -1)
    inverse = lax.rsqrt(jnp.mean(inputs * inputs, axis=1, keepdims=True) + 1e-06)
    normed = (inputs * inverse * norm_gain).astype(jnp.bfloat16)
    lowered = jnp.dot(normed, local_down, preferred_element_type=jnp.float32)
    byte_tasks = jnp.repeat(tasks, PATCH)
    scales = select_rows(local_scales, byte_tasks)
    shrunk = (lowered * scales).astype(jnp.bfloat16)
    return (inputs, inverse, normed, lowered, scales, shrunk, byte_tasks)


def keep_state(current):
    return current


def update_state(state, query_rows, first, key_heads, value_heads, key_places, scale):
    running_max, running_sum, running_out = state
    count = query_rows.shape[0]
    heads = key_heads.shape[1]
    query_heads = query_rows.reshape(count, heads, HEAD)
    scores = (
        jnp.einsum("qhd,khd->hqk", query_heads, key_heads, preferred_element_type=jnp.float32)
        * scale
    )
    query_places = first + jnp.arange(count, dtype=jnp.int32)
    allowed = key_places[None, :] <= query_places[:, None]
    scores = jnp.where(allowed[None], scores, -1e30)
    new_max = jnp.maximum(running_max, jnp.max(scores, axis=2))
    weights = jnp.where(allowed[None], jnp.exp(scores - new_max[:, :, None]), 0.0)
    shrink = jnp.exp(running_max - new_max)
    running_sum = running_sum * shrink + jnp.sum(weights, axis=2)
    mixed = jnp.einsum(
        "hqk,khd->qhd",
        weights.astype(jnp.bfloat16),
        value_heads,
        preferred_element_type=jnp.float32,
    )
    running_out = running_out * jnp.transpose(shrink)[:, :, None] + mixed
    return (new_max, running_sum, running_out)


def finish_state(state):
    running_max, running_sum, running_out = state
    result = running_out / jnp.transpose(running_sum)[:, :, None]
    return result.reshape(result.shape[0], -1).astype(jnp.bfloat16)


def general_body(
    patch_queries,
    patch_keys,
    patch_values,
    patch_tasks,
    residual,
    output_weight,
    global_down,
    global_up,
    global_scales,
    local_weight,
    byte_ids,
    byte_table,
    position_table,
    norm_gain,
    hidden_in,
    hidden_out,
    local_down,
    local_up,
    local_scales,
    cotangent,
):
    rows = patch_queries.shape[0]
    width = patch_queries.shape[1]
    heads = width // HEAD
    row_count = lax.axis_size("row")
    seq_index = lax.axis_index("seq")
    row_index = lax.axis_index("row")
    scale = 1.0 / math.sqrt(HEAD)
    own_first = seq_index * rows
    groups = [(patch_queries, own_first)]

    def visit(state, query_rows, first, key_heads, value_heads, key_places):

        def refresh(current):
            return update_state(
                current, query_rows, first, key_heads, value_heads, key_places, scale
            )

        return lax.cond(
            key_places[0] <= first + query_rows.shape[0] - 1, refresh, keep_state, state
        )

    initial = tuple(
        (
            (
                jnp.full((heads, query_rows.shape[0]), -1e30, jnp.float32),
                jnp.zeros((heads, query_rows.shape[0]), jnp.float32),
                jnp.zeros((query_rows.shape[0], heads, HEAD), jnp.float32),
            )
            for query_rows, first in groups
        )
    )
    key_piece = lax.all_gather(patch_keys, "seq", axis=0, tiled=True)
    value_piece = lax.all_gather(patch_values, "seq", axis=0, tiled=True)
    count = key_piece.shape[0]
    span = math.gcd(count, 1024)

    def one_span(index, states):
        offset = index * span
        key_heads = lax.dynamic_slice_in_dim(key_piece, offset, span, 0).reshape(span, heads, HEAD)
        value_heads = lax.dynamic_slice_in_dim(value_piece, offset, span, 0).reshape(
            span, heads, HEAD
        )
        key_places = offset + jnp.arange(span, dtype=jnp.int32)
        updated = []
        for (query_rows, first), state in zip(groups, states):
            updated.append(visit(state, query_rows, first, key_heads, value_heads, key_places))
        return tuple(updated)

    states = lax.fori_loop(0, count // span, one_span, initial)
    outputs = [finish_state(state) for state in states]
    attended = outputs[0]
    reduced = lax.psum(jnp.dot(attended, global_down, preferred_element_type=jnp.float32), "row")
    task_scales = select_rows(global_scales, patch_tasks)
    scaled = (reduced * task_scales).astype(jnp.bfloat16)
    mixed = lax.psum_scatter(
        contract(output_weight, attended, 0, 1).astype(jnp.bfloat16),
        "row",
        scatter_dimension=0,
        tiled=True,
    ).astype(jnp.float32)
    mixed = mixed + jnp.transpose(residual.astype(jnp.float32)) + contract(global_up, scaled, 0, 1)
    mixed_b = mixed.astype(jnp.bfloat16)
    own_patches = rows // row_count
    own_bytes = own_patches * PATCH
    rows_in, rows_out = (
        lax.all_gather(hidden_in, "seq", axis=1, tiled=True),
        lax.all_gather(hidden_out, "seq", axis=1, tiled=True),
    )
    partial_value = contract(mixed_b, local_weight, 0, 0)
    projected = lax.psum(partial_value.astype(jnp.bfloat16), "row")
    every = local_inputs(
        byte_ids,
        projected,
        patch_tasks,
        byte_table,
        position_table,
        norm_gain,
        local_down,
        local_scales,
    )
    normed_all = every[2]
    shrunk_all = every[5]
    cotangent_all = lax.all_gather(cotangent, "row", axis=0, tiled=True)
    inputs, inverse, normed, lowered, scales, shrunk, byte_tasks = [
        lax.dynamic_slice_in_dim(value, row_index * own_bytes, own_bytes, 0) for value in every
    ]
    upper = contract(normed_all, rows_in, 1, 1) + jnp.dot(
        shrunk_all, local_up, preferred_element_type=jnp.float32
    )
    through = contract(cotangent_all, rows_out, 1, 1)
    grown = (through * gelu_slope(upper)).astype(jnp.bfloat16)
    grad_local_up = contract(shrunk_all, grown, 0, 0)
    back_norm, back_rank = (
        lax.psum_scatter(
            jnp.dot(grown, rows_in, preferred_element_type=jnp.float32).astype(jnp.bfloat16),
            "row",
            scatter_dimension=0,
            tiled=True,
        ).astype(jnp.float32),
        lax.psum_scatter(
            contract(grown, local_up, 1, 1).astype(jnp.bfloat16),
            "row",
            scatter_dimension=0,
            tiled=True,
        ).astype(jnp.float32),
    )
    grad_local_scales = task_totals(byte_tasks, back_rank * lowered)
    moved = (back_rank * scales).astype(jnp.bfloat16)
    grad_local_down = contract(normed, moved, 0, 0)
    back_total = back_norm + contract(moved, local_down, 1, 1)
    gained = back_total * norm_gain
    average = jnp.mean(gained * inputs, axis=1, keepdims=True)
    back_inputs = cotangent.astype(jnp.float32) + inverse * (
        gained - inputs * inverse * inverse * average
    )
    patch_grad = back_inputs.reshape(own_patches, PATCH, -1).sum(axis=1).astype(jnp.bfloat16)
    back_mixed = contract(
        lax.all_gather(patch_grad, "row", axis=0, tiled=True), local_weight, 1, 1
    ).astype(jnp.bfloat16)
    grad_global_up = contract(scaled, back_mixed, 0, 0)
    back_scaled = lax.psum(contract(back_mixed, global_up, 1, 1), "row")
    grad_global_scales = task_totals(patch_tasks, back_scaled * reduced)
    back_reduced = (back_scaled * task_scales).astype(jnp.bfloat16)
    grad_global_down = contract(attended, back_reduced, 0, 0)
    grad_global_down, grad_global_up, grad_global_scales, grad_local_up = lax.psum(
        (grad_global_down, grad_global_up, grad_global_scales, grad_local_up), "seq"
    )
    grad_local_down, grad_local_scales = lax.psum(
        (grad_local_down, grad_local_scales), ("seq", "row")
    )
    return (
        grad_global_down,
        grad_global_up,
        grad_global_scales,
        grad_local_down,
        grad_local_up,
        grad_local_scales,
    )


MESH = pl.DeviceIdType.MESH


def remote(src, dst, send, recv, seq, row):
    return pltpu.make_async_remote_copy(
        src_ref=src,
        dst_ref=dst,
        send_sem=send,
        recv_sem=recv,
        device_id=(seq, row),
        device_id_type=MESH,
    )


def greet(peers):
    barrier = pltpu.get_barrier_semaphore()
    for seq, row in peers:
        pl.semaphore_signal(barrier, inc=1, device_id=(seq, row), device_id_type=MESH)
    pl.semaphore_wait(barrier, len(peers))


def front_kernel(
    chips, depth, q_ref, k_ref, v_ref, w_ref, cot_ref, ow_ref, lw_ref, gd_ref, gu_ref, res_ref,
    att_out, proj_out, m_out, w_out, cot_out,
    qb, kb, vb, ob, att, wb, cotb, lwb, w2, acc, e1, e1r, mb, mr,
    a_send, a_recv, f_send, f_recv, o_send, o_recv, z_send, z_recv, x_send, x_recv,
    p_send, p_recv, c_send, c_recv, y_send, y_recv,
):
    me = lax.axis_index("seq")
    row = lax.axis_index("row")
    other = 1 - row
    chip, core = me // 2, lax.rem(me, 2)
    mate = 2 * chip + (1 - core)
    rows = q_ref.shape[0]
    half = lw_ref.shape[0] // 2

    def at(number):
        return lax.rem(number + 2 * chips, chips)

    def heads_of(number):
        return pl.ds(pl.multiple_of(number * HEAD, HEAD), HEAD)

    greet([(2 * at(chip + d) + core, row) for d in range(1, chips)] + [(mate, row), (me, other)])

    own = heads_of(chip)
    sends = []
    arrivals = {}
    own_half = pl.ds(pl.multiple_of(core * half, half), half)
    mate_half = pl.ds(pl.multiple_of((1 - core) * half, half), half)
    lw_copy = remote(lw_ref.at[own_half], lwb.at[own_half], y_send.at[0], y_recv.at[0], me, other)
    lw_copy.start()
    forwards = {}
    order = sorted(range(1, chips), key=lambda d: -min(d, chips - d))
    for d in order:
        to = at(chip + d)
        for which, (src, dst) in enumerate(
            ((k_ref, kb.at[me]), (v_ref, vb.at[me]), (q_ref, qb.at[chip]))
        ):
            copy = remote(
                src.at[:, heads_of(to)], dst, a_send.at[which, d], a_recv.at[which, d],
                2 * to + core, row,
            )
            copy.start()
            arrivals[which, d] = copy
    for which, (src, dst) in enumerate(((k_ref, kb), (v_ref, vb))):
        copy = remote(
            src.at[:, own], dst.at[me], f_send.at[which, 0], f_recv.at[which, 0], mate, row
        )
        copy.start()
        forwards[which, 0] = copy
    cot_copy = remote(cot_ref, cotb, c_send.at[0], c_recv.at[0], me, other)
    cot_copy.start()

    levels = chips // depth
    level, side = chip // depth, lax.rem(chip, depth)
    z_copies = []
    for d in range(1, levels):
        to = lax.rem(level + d, levels) * depth + side
        copy = remote(w_ref, wb.at[me], z_send.at[d], z_recv.at[d], 2 * to + core, row)
        copy.start()
        z_copies.append((d, copy))
    neighbour = 2 * (level * depth + (1 - side)) + core
    x_copies = []
    p_copies = []

    def pass_side(d, src, slot):
        copy = remote(src, wb.at[slot], x_send.at[d], x_recv.at[d], neighbour, row)
        copy.start()
        x_copies.append((d, copy))

    def pass_mate(number, src, slot):
        copy = remote(src, wb.at[slot], p_send.at[number], p_recv.at[number], mate, row)
        copy.start()
        p_copies.append(copy)

    pass_side(0, w_ref, me)
    pass_mate(0, w_ref, me)

    qb[chip] = q_ref[:, own]
    kb[me] = k_ref[:, own]
    vb[me] = v_ref[:, own]
    wb[me] = w_ref[...]

    mb[...] = jnp.dot(
        gu_ref[...], lw_ref[...], preferred_element_type=jnp.float32
    ).astype(jnp.bfloat16)
    m_copy = remote(mb, mr, y_send.at[2], y_recv.at[2], me, other)
    m_copy.start()

    width = lw_ref.shape[0]
    tile = math.gcd(ow_ref.shape[0], 256)
    columns = lw_ref.shape[1]

    @pl.loop(0, ow_ref.shape[0] // tile)
    def _(index):
        part = pl.ds(pl.multiple_of(index * tile, tile), tile)
        acc[part] = jnp.dot(
            ow_ref[part, pl.ds(pl.multiple_of(row * width, width), width)],
            lw_ref[...],
            preferred_element_type=jnp.float32,
        )

    lw_copy.wait_recv()
    lw_mate = remote(lwb.at[own_half], lwb.at[own_half], y_send.at[1], y_recv.at[1], mate, row)
    lw_mate.start()
    lw_mate.wait_recv()

    @pl.loop(0, ow_ref.shape[0] // tile)
    def _(index):
        part = pl.ds(pl.multiple_of(index * tile, tile), tile)
        total = acc[part] + jnp.dot(
            ow_ref[part, pl.ds(pl.multiple_of(other * width, width), width)],
            lwb[...],
            preferred_element_type=jnp.float32,
        )
        w2[part, :columns] = total.astype(jnp.bfloat16)
        w2[part, columns:] = gd_ref[part]

    for d in reversed(range(1, chips)):
        for which, buffer in ((0, kb), (1, vb)):
            arrivals[which, d].wait_recv()
            slot = 2 * at(chip - d) + core
            copy = remote(
                buffer.at[slot], buffer.at[slot], f_send.at[which, d], f_recv.at[which, d],
                mate, row,
            )
            copy.start()
            forwards[which, d] = copy
        arrivals[2, d].wait_recv()
    for copy in forwards.values():
        copy.wait_recv()

    scale = 1.0 / math.sqrt(HEAD)
    for i in reversed(range(chips)):
        span = (2 * i + 2) * rows
        keys = kb[: 2 * i + 2].reshape(span, HEAD)
        values = vb[: 2 * i + 2].reshape(span, HEAD)
        scores = contract(qb[i], keys, 1, 1) * scale
        last = 2 * rows
        places = lax.broadcasted_iota(jnp.int32, (rows, span), 1)
        queries = lax.broadcasted_iota(jnp.int32, (rows, span), 0) + (2 * i + core) * rows
        scores = jnp.where(places <= queries, scores, -1e30)
        top = jnp.max(scores, axis=1, keepdims=True)
        weights = jnp.exp(scores - top)
        mass = jnp.sum(weights, axis=1, keepdims=True)
        mixed = jnp.dot(weights.astype(jnp.bfloat16), values, preferred_element_type=jnp.float32)
        ob[i] = (mixed / mass).astype(jnp.bfloat16)

        @pl.when(i != chip)
        def _():
            remote(
                ob.at[i], att.at[:, own], o_send.at[i], o_recv.at[chip], 2 * i + core, row
            ).start()

        @pl.when(i == chip)
        def _():
            att[:, own] = ob[i]

    for d, copy in z_copies:
        copy.wait_recv()
        slot = 2 * (lax.rem(level - d + levels, levels) * depth + side) + core
        pass_side(d, wb.at[slot], slot)
        pass_mate(d, wb.at[slot], slot)
    for d, copy in list(x_copies):
        copy.wait_recv()
        slot = 2 * (lax.rem(level - d + levels, levels) * depth + (1 - side)) + core
        pass_mate(levels + d, wb.at[slot], slot)

    for i in range(chips):

        @pl.when(i != chip)
        def _():
            back = remote(
                ob.at[i], att.at[:, heads_of(i)], o_send.at[i], o_recv.at[i], 2 * i + core, row
            )
            back.wait_recv()
            back.wait_send()

    value = jnp.dot(att[...], w2[...], preferred_element_type=jnp.float32)
    e1[:, :columns] = (
        value[:, :columns]
        + jnp.dot(res_ref[...], lw_ref[...], preferred_element_type=jnp.float32)
    ).astype(jnp.bfloat16)
    e1[:, columns:] = value[:, columns:].astype(jnp.bfloat16)
    e_copy = remote(e1, e1r, y_send.at[3], y_recv.at[3], me, other)
    e_copy.start()
    att_out[...] = att[...]
    cot_copy.wait_recv()
    cot_out[row] = cot_ref[...]
    cot_out[other] = cotb[...]
    m_copy.wait_recv()
    m_out[...] = mb[...].astype(jnp.float32) + mr[...].astype(jnp.float32)
    for copy in p_copies:
        copy.wait_recv()
    shard = w_ref.shape[0] // 2
    w_out[0] = wb[:, :shard]
    w_out[1] = wb[:, shard:]
    e_copy.wait_recv()
    proj_out[...] = e1[...].astype(jnp.float32) + e1r[...].astype(jnp.float32)
    for copy in (
        [lw_copy, lw_mate, cot_copy, m_copy, e_copy]
        + list(arrivals.values())
        + list(forwards.values())
        + [copy for d, copy in z_copies + x_copies]
        + p_copies
    ):
        copy.wait_send()


def front(q, k, v, w, cot, ow, lw, gd, gu, res, count):
    chips = q.shape[1] // HEAD
    rows = q.shape[0]
    depth = 2
    levels = chips // depth
    columns = lw.shape[1]
    wide = columns + gd.shape[1]
    vm = pl.BlockSpec(memory_space=pltpu.VMEM)
    dma = pltpu.SemaphoreType.DMA
    bf, f32 = jnp.bfloat16, jnp.float32
    return pl.pallas_call(
        functools.partial(front_kernel, chips, depth),
        out_shape=(
            jax.ShapeDtypeStruct(q.shape, bf),
            jax.ShapeDtypeStruct((rows, wide), f32),
            jax.ShapeDtypeStruct((gu.shape[0], columns), f32),
            jax.ShapeDtypeStruct((2, count, w.shape[0] // 2, w.shape[1]), bf),
            jax.ShapeDtypeStruct((2,) + cot.shape, bf),
        ),
        in_specs=[vm] * 10,
        out_specs=(vm,) * 5,
        scratch_shapes=[
            pltpu.VMEM((chips, rows, HEAD), bf),
            pltpu.VMEM((count, rows, HEAD), bf),
            pltpu.VMEM((count, rows, HEAD), bf),
            pltpu.VMEM((chips, rows, HEAD), bf),
            pltpu.VMEM(q.shape, bf),
            pltpu.VMEM((count,) + w.shape, bf),
            pltpu.VMEM(cot.shape, bf),
            pltpu.VMEM(lw.shape, bf),
            pltpu.VMEM((ow.shape[0], wide), bf),
            pltpu.VMEM((ow.shape[0], columns), f32),
            pltpu.VMEM((rows, wide), bf),
            pltpu.VMEM((rows, wide), bf),
            pltpu.VMEM((gu.shape[0], columns), bf),
            pltpu.VMEM((gu.shape[0], columns), bf),
            dma((3, chips)), dma((3, chips)),
            dma((2, chips)), dma((2, chips)),
            dma((chips,)), dma((chips,)),
            dma((levels,)), dma((levels,)),
            dma((levels,)), dma((levels,)),
            dma((chips,)), dma((chips,)),
            dma((1,)), dma((1,)),
            dma((4,)), dma((4,)),
        ],
        compiler_params=pltpu.CompilerParams(
            collective_id=0, has_side_effects=True, vmem_limit_bytes=60 * 1024 * 1024
        ),
        name="front",
    )(q, k, v, w, cot, ow, lw, gd, gu, res)


def swap_kernel(x_ref, o_ref, buf, send, recv):
    me, row = lax.axis_index("seq"), lax.axis_index("row")
    greet([(me, 1 - row)])
    copy = remote(x_ref, buf, send, recv, me, 1 - row)
    copy.start()
    copy.wait()
    o_ref[...] = x_ref[...].astype(jnp.float32) + buf[...].astype(jnp.float32)


def row_sum(x):
    vm = pl.BlockSpec(memory_space=pltpu.VMEM)
    return pl.pallas_call(
        swap_kernel,
        out_shape=jax.ShapeDtypeStruct(x.shape, jnp.float32),
        in_specs=[vm],
        out_specs=vm,
        scratch_shapes=[
            pltpu.VMEM(x.shape, x.dtype), pltpu.SemaphoreType.DMA, pltpu.SemaphoreType.DMA
        ],
        compiler_params=pltpu.CompilerParams(collective_id=1, has_side_effects=True),
        name="row_sum",
    )(x)


def total_kernel(count, shared, g_ref, o_ref, part, result, full, s1, r1, s2, r2, s3, r3):
    me, row = lax.axis_index("seq"), lax.axis_index("row")
    other = 1 - row
    peers = [(lax.rem(me + d, count), row) for d in range(1, count)]
    cross = [(lax.rem(me + d, count), other) for d in range(count)]
    greet(peers + cross)
    first = []
    for d in range(1, count):
        to = lax.rem(me + d, count)
        copy = remote(g_ref.at[to], part.at[row, me], s1.at[d], r1.at[d], to, row)
        copy.start()
        first.append(copy)
    crossing = []
    for index, to in enumerate(shared):
        copy = remote(g_ref.at[to], part.at[row, me], s3.at[index], r3.at[me], to, other)
        copy.start()
        crossing.append(copy)
    part[row, me] = g_ref[me]
    for copy in first:
        copy.wait_recv()

    def add(side):
        return jnp.sum(part[side].astype(jnp.float32), axis=0)

    result[...] = add(row).astype(jnp.bfloat16)

    @pl.when(me >= shared[0])
    def _():
        for source in range(count):
            remote(
                g_ref.at[0], part.at[other, source], s3.at[0], r3.at[source], me, other
            ).wait_recv()
        result[...] = (add(0) + add(1)).astype(jnp.bfloat16)

    second = []
    for d in range(1, count):
        to = lax.rem(me + d, count)
        copy = remote(result, full.at[me], s2.at[d], r2.at[d], to, row)
        copy.start()
        second.append(copy)
    full[me] = result[...]
    for copy in second:
        copy.wait_recv()
    o_ref[...] = full[...].astype(jnp.float32)
    for copy in first + crossing + second:
        copy.wait_send()


def grand_total(g, shared):
    count = g.shape[0]
    vm = pl.BlockSpec(memory_space=pltpu.VMEM)
    dma = pltpu.SemaphoreType.DMA
    return pl.pallas_call(
        functools.partial(total_kernel, count, shared),
        out_shape=jax.ShapeDtypeStruct(g.shape, jnp.float32),
        in_specs=[vm],
        out_specs=vm,
        scratch_shapes=[
            pltpu.VMEM((2,) + g.shape, g.dtype),
            pltpu.VMEM(g.shape[1:], g.dtype),
            pltpu.VMEM(g.shape, g.dtype),
            dma((count,)), dma((count,)),
            dma((count,)), dma((count,)),
            dma((len(shared),)), dma((count,)),
        ],
        compiler_params=pltpu.CompilerParams(collective_id=2, has_side_effects=True),
        name="grand_total",
    )(g)


def paired_body(
    patch_queries,
    patch_keys,
    patch_values,
    patch_tasks,
    residual,
    output_weight,
    global_down,
    global_up,
    global_scales,
    local_weight,
    byte_ids,
    byte_table,
    position_table,
    norm_gain,
    hidden_in,
    hidden_out,
    local_down,
    local_up,
    local_scales,
    cotangent,
):
    count = lax.axis_size("seq")
    bf = jnp.bfloat16
    rank = global_up.shape[0]
    columns = local_weight.shape[1]
    hidden = hidden_in.shape[0]
    shards = jnp.concatenate([jnp.transpose(hidden_in), jnp.transpose(hidden_out)], axis=0)
    wide_down = jnp.pad(global_down, ((0, 0), (0, HEAD - rank)))
    attended, proj, bridge, weights, cot = front(
        patch_queries, patch_keys, patch_values, shards, cotangent, output_weight,
        local_weight, wide_down, global_up, residual, count,
    )
    reduced = proj[:, columns : columns + rank]
    rows_in = weights[0].reshape(columns, hidden)
    rows_out = weights[1].reshape(columns, hidden)
    cot = cot.reshape(-1, columns)
    task_scales = select_rows(global_scales, patch_tasks)
    scaled = (reduced * task_scales).astype(bf)
    bridge_b = bridge.astype(bf)
    projected = (
        proj[:, :columns] + jnp.dot(scaled, bridge_b, preferred_element_type=jnp.float32)
    ).astype(bf)
    inputs, inverse, normed, lowered, scales, shrunk, byte_tasks = local_inputs(
        byte_ids, projected, patch_tasks, byte_table, position_table, norm_gain, local_down,
        local_scales,
    )
    upper = jnp.dot(normed, rows_in, preferred_element_type=jnp.float32) + jnp.dot(
        shrunk, local_up, preferred_element_type=jnp.float32
    )
    through = jnp.dot(cot, rows_out, preferred_element_type=jnp.float32)
    grown = (through * gelu_slope(upper)).astype(bf)
    grad_local_up = contract(shrunk, grown, 0, 0)
    back_rank = contract(grown, local_up, 1, 1)
    moved = (back_rank * scales).astype(bf)
    grad_local_scales = task_totals(byte_tasks, back_rank * lowered)
    grad_local_down = contract(moved, normed, 0, 0)
    back_total = contract(grown, rows_in, 1, 1) + contract(moved, local_down, 1, 1)
    gained = back_total * norm_gain
    average = jnp.mean(gained * inputs, axis=1, keepdims=True)
    back_inputs = inverse * (gained - inputs * inverse * inverse * average)
    patches = patch_tasks.shape[0]
    back_part = back_inputs.reshape(patches, PATCH, -1).sum(axis=1).astype(bf)
    cot_sum = cot.astype(jnp.float32).reshape(patches, PATCH, -1).sum(axis=1)
    patch_grad = (row_sum(back_part) + cot_sum).astype(bf)
    back_mixed = contract(patch_grad, local_weight, 1, 1).astype(bf)
    grad_global_up = contract(scaled, back_mixed, 0, 0)
    back_scaled = contract(patch_grad, bridge_b, 1, 1)
    grad_global_scales = task_totals(patch_tasks, back_scaled * reduced)
    back_reduced = (back_scaled * task_scales).astype(bf)
    grad_global_down = contract(back_reduced, attended, 0, 0)

    spare = hidden - columns - rank
    small = jnp.concatenate([0.5 * grad_global_scales, grad_local_scales], axis=0)
    last = jnp.concatenate(
        [grad_local_down, small, jnp.zeros((rank, spare), jnp.float32)], axis=1
    )
    packed = jnp.concatenate(
        [grad_global_down, grad_global_up, grad_local_up, last], axis=0
    ).astype(bf)
    blocks = packed.reshape(count, 16, -1)
    shared = tuple(range(count - count // 4, count))
    summed = grand_total(blocks, shared).reshape(packed.shape)
    last = summed[3 * rank :]
    return (
        jnp.transpose(summed[:rank]),
        summed[rank : 2 * rank],
        last[:TASKS, columns : columns + rank],
        jnp.transpose(last[:, :columns]),
        summed[2 * rank : 3 * rank],
        last[TASKS:, columns : columns + rank],
    )


def pick_body(seq_count, row_count, *args):
    heads = args[0].shape[1] // HEAD
    rank = args[7].shape[0]
    hidden = args[14].shape[0]
    fits = (
        row_count == 2
        and seq_count == 2 * heads
        and heads % 4 == 0
        and rank == 2 * TASKS
        and args[0].shape[1] == hidden
        and (4 * rank * hidden) % (seq_count * 16 * HEAD) == 0
        and hidden >= args[9].shape[1] + rank
    )
    return paired_body(*args) if fits else general_body(*args)


def solution(mesh):
    placed = (
        P("seq", "row"),
        P("seq", "row"),
        P("seq", "row"),
        P("seq"),
        P("seq", "row"),
        P("row", None),
        P("row", None),
        P(None, "row"),
        P(),
        P("row", None),
        P("seq"),
        P(),
        P(),
        P(),
        P("row", "seq"),
        P("row", "seq"),
        P(),
        P(None, "row"),
        P(),
        P(("seq", "row"), None),
    )
    chosen = functools.partial(pick_body, mesh.shape["seq"], mesh.shape["row"])
    return jax.shard_map(
        chosen,
        mesh=mesh,
        in_specs=placed,
        out_specs=(P("row", None), P(None, "row"), P(), P(), P(None, "row"), P()),
        check_vma=False,
    )
```

```python
import functools
import math

import jax
import jax.numpy as jnp
from jax import lax
from jax.experimental import pallas as pl
from jax.experimental.pallas import tpu as pltpu
from jax.sharding import PartitionSpec as P

HEAD = 128
VOCAB = 256
PATCH = 8
TASKS = 8


def contract(left, right, left_dim, right_dim):
    return lax.dot_general(
        left, right, (((left_dim,), (right_dim,)), ((), ())), preferred_element_type=jnp.float32
    )


def select_rows(table, tasks):
    picks = (tasks[:, None] == jnp.arange(table.shape[0], dtype=jnp.int32)[None, :]).astype(
        jnp.float32
    )
    return jnp.dot(picks, table, precision=lax.Precision.HIGHEST)


def task_totals(tasks, values):
    picks = (tasks[:, None] == jnp.arange(TASKS, dtype=jnp.int32)[None, :]).astype(jnp.float32)
    return lax.dot_general(picks, values, (((0,), (0,)), ((), ())), precision=lax.Precision.HIGHEST)


def gelu_slope(upper):
    cumulative = 0.5 * (1.0 + lax.erf(upper * 0.7071067811865476))
    density = jnp.exp(-0.5 * upper * upper) * 0.3989422804014327
    return cumulative + upper * density


def local_inputs(
    identities, projected, tasks, byte_table, position_table, norm_gain, local_down, local_scales
):
    count = identities.shape[0]
    picks = (identities[:, None] == jnp.arange(VOCAB, dtype=jnp.int32)[None, :]).astype(
        jnp.bfloat16
    )
    embedded = jnp.dot(picks, byte_table, preferred_element_type=jnp.float32)
    patches = count // PATCH
    inputs = (
        embedded.reshape(patches, PATCH, -1)
        + position_table.astype(jnp.float32)[None]
        + projected.astype(jnp.float32)[:, None, :]
    )
    inputs = inputs.reshape(count, -1)
    inverse = lax.rsqrt(jnp.mean(inputs * inputs, axis=1, keepdims=True) + 1e-06)
    normed = (inputs * inverse * norm_gain).astype(jnp.bfloat16)
    lowered = jnp.dot(normed, local_down, preferred_element_type=jnp.float32)
    byte_tasks = jnp.repeat(tasks, PATCH)
    scales = select_rows(local_scales, byte_tasks)
    shrunk = (lowered * scales).astype(jnp.bfloat16)
    return (inputs, inverse, normed, lowered, scales, shrunk, byte_tasks)


def keep_state(current):
    return current


def update_state(state, query_rows, first, key_heads, value_heads, key_places, scale):
    running_max, running_sum, running_out = state
    count = query_rows.shape[0]
    heads = key_heads.shape[1]
    query_heads = query_rows.reshape(count, heads, HEAD)
    scores = (
        jnp.einsum("qhd,khd->hqk", query_heads, key_heads, preferred_element_type=jnp.float32)
        * scale
    )
    query_places = first + jnp.arange(count, dtype=jnp.int32)
    allowed = key_places[None, :] <= query_places[:, None]
    scores = jnp.where(allowed[None], scores, -1e30)
    new_max = jnp.maximum(running_max, jnp.max(scores, axis=2))
    weights = jnp.where(allowed[None], jnp.exp(scores - new_max[:, :, None]), 0.0)
    shrink = jnp.exp(running_max - new_max)
    running_sum = running_sum * shrink + jnp.sum(weights, axis=2)
    mixed = jnp.einsum(
        "hqk,khd->qhd",
        weights.astype(jnp.bfloat16),
        value_heads,
        preferred_element_type=jnp.float32,
    )
    running_out = running_out * jnp.transpose(shrink)[:, :, None] + mixed
    return (new_max, running_sum, running_out)


def finish_state(state):
    running_max, running_sum, running_out = state
    result = running_out / jnp.transpose(running_sum)[:, :, None]
    return result.reshape(result.shape[0], -1).astype(jnp.bfloat16)


def general_body(
    patch_queries,
    patch_keys,
    patch_values,
    patch_tasks,
    residual,
    output_weight,
    global_down,
    global_up,
    global_scales,
    local_weight,
    byte_ids,
    byte_table,
    position_table,
    norm_gain,
    hidden_in,
    hidden_out,
    local_down,
    local_up,
    local_scales,
    cotangent,
):
    rows = patch_queries.shape[0]
    width = patch_queries.shape[1]
    heads = width // HEAD
    row_count = lax.axis_size("row")
    seq_index = lax.axis_index("seq")
    row_index = lax.axis_index("row")
    scale = 1.0 / math.sqrt(HEAD)
    own_first = seq_index * rows
    groups = [(patch_queries, own_first)]

    def visit(state, query_rows, first, key_heads, value_heads, key_places):

        def refresh(current):
            return update_state(
                current, query_rows, first, key_heads, value_heads, key_places, scale
            )

        return lax.cond(
            key_places[0] <= first + query_rows.shape[0] - 1, refresh, keep_state, state
        )

    initial = tuple(
        (
            (
                jnp.full((heads, query_rows.shape[0]), -1e30, jnp.float32),
                jnp.zeros((heads, query_rows.shape[0]), jnp.float32),
                jnp.zeros((query_rows.shape[0], heads, HEAD), jnp.float32),
            )
            for query_rows, first in groups
        )
    )
    key_piece = lax.all_gather(patch_keys, "seq", axis=0, tiled=True)
    value_piece = lax.all_gather(patch_values, "seq", axis=0, tiled=True)
    count = key_piece.shape[0]
    span = math.gcd(count, 1024)

    def one_span(index, states):
        offset = index * span
        key_heads = lax.dynamic_slice_in_dim(key_piece, offset, span, 0).reshape(span, heads, HEAD)
        value_heads = lax.dynamic_slice_in_dim(value_piece, offset, span, 0).reshape(
            span, heads, HEAD
        )
        key_places = offset + jnp.arange(span, dtype=jnp.int32)
        updated = []
        for (query_rows, first), state in zip(groups, states):
            updated.append(visit(state, query_rows, first, key_heads, value_heads, key_places))
        return tuple(updated)

    states = lax.fori_loop(0, count // span, one_span, initial)
    outputs = [finish_state(state) for state in states]
    attended = outputs[0]
    reduced = lax.psum(jnp.dot(attended, global_down, preferred_element_type=jnp.float32), "row")
    task_scales = select_rows(global_scales, patch_tasks)
    scaled = (reduced * task_scales).astype(jnp.bfloat16)
    mixed = lax.psum_scatter(
        contract(output_weight, attended, 0, 1).astype(jnp.bfloat16),
        "row",
        scatter_dimension=0,
        tiled=True,
    ).astype(jnp.float32)
    mixed = mixed + jnp.transpose(residual.astype(jnp.float32)) + contract(global_up, scaled, 0, 1)
    mixed_b = mixed.astype(jnp.bfloat16)
    own_patches = rows // row_count
    own_bytes = own_patches * PATCH
    rows_in, rows_out = (
        lax.all_gather(hidden_in, "seq", axis=1, tiled=True),
        lax.all_gather(hidden_out, "seq", axis=1, tiled=True),
    )
    partial_value = contract(mixed_b, local_weight, 0, 0)
    projected = lax.psum(partial_value.astype(jnp.bfloat16), "row")
    every = local_inputs(
        byte_ids,
        projected,
        patch_tasks,
        byte_table,
        position_table,
        norm_gain,
        local_down,
        local_scales,
    )
    normed_all = every[2]
    shrunk_all = every[5]
    cotangent_all = lax.all_gather(cotangent, "row", axis=0, tiled=True)
    inputs, inverse, normed, lowered, scales, shrunk, byte_tasks = [
        lax.dynamic_slice_in_dim(value, row_index * own_bytes, own_bytes, 0) for value in every
    ]
    upper = contract(normed_all, rows_in, 1, 1) + jnp.dot(
        shrunk_all, local_up, preferred_element_type=jnp.float32
    )
    through = contract(cotangent_all, rows_out, 1, 1)
    grown = (through * gelu_slope(upper)).astype(jnp.bfloat16)
    grad_local_up = contract(shrunk_all, grown, 0, 0)
    back_norm, back_rank = (
        lax.psum_scatter(
            jnp.dot(grown, rows_in, preferred_element_type=jnp.float32).astype(jnp.bfloat16),
            "row",
            scatter_dimension=0,
            tiled=True,
        ).astype(jnp.float32),
        lax.psum_scatter(
            contract(grown, local_up, 1, 1).astype(jnp.bfloat16),
            "row",
            scatter_dimension=0,
            tiled=True,
        ).astype(jnp.float32),
    )
    grad_local_scales = task_totals(byte_tasks, back_rank * lowered)
    moved = (back_rank * scales).astype(jnp.bfloat16)
    grad_local_down = contract(normed, moved, 0, 0)
    back_total = back_norm + contract(moved, local_down, 1, 1)
    gained = back_total * norm_gain
    average = jnp.mean(gained * inputs, axis=1, keepdims=True)
    back_inputs = cotangent.astype(jnp.float32) + inverse * (
        gained - inputs * inverse * inverse * average
    )
    patch_grad = back_inputs.reshape(own_patches, PATCH, -1).sum(axis=1).astype(jnp.bfloat16)
    back_mixed = contract(
        lax.all_gather(patch_grad, "row", axis=0, tiled=True), local_weight, 1, 1
    ).astype(jnp.bfloat16)
    grad_global_up = contract(scaled, back_mixed, 0, 0)
    back_scaled = lax.psum(contract(back_mixed, global_up, 1, 1), "row")
    grad_global_scales = task_totals(patch_tasks, back_scaled * reduced)
    back_reduced = (back_scaled * task_scales).astype(jnp.bfloat16)
    grad_global_down = contract(attended, back_reduced, 0, 0)
    grad_global_down, grad_global_up, grad_global_scales, grad_local_up = lax.psum(
        (grad_global_down, grad_global_up, grad_global_scales, grad_local_up), "seq"
    )
    grad_local_down, grad_local_scales = lax.psum(
        (grad_local_down, grad_local_scales), ("seq", "row")
    )
    return (
        grad_global_down,
        grad_global_up,
        grad_global_scales,
        grad_local_down,
        grad_local_up,
        grad_local_scales,
    )


MESH = pl.DeviceIdType.MESH


def remote(src, dst, send, recv, seq, row):
    return pltpu.make_async_remote_copy(
        src_ref=src,
        dst_ref=dst,
        send_sem=send,
        recv_sem=recv,
        device_id=(seq, row),
        device_id_type=MESH,
    )


def greet(peers):
    barrier = pltpu.get_barrier_semaphore()
    for seq, row in peers:
        pl.semaphore_signal(barrier, inc=1, device_id=(seq, row), device_id_type=MESH)
    pl.semaphore_wait(barrier, len(peers))


def front_kernel(
    chips, depth, q_ref, k_ref, v_ref, hi_ref, ho_ref, cot_ref, ow_hbm, lw_ref, gd_ref, gu_ref,
    res_ref, att_out, proj_out, m_out, hi_out, ho_out, cot_out,
    ow_ref, ow_sem, qb, kb, vb, ob, att, wb, cotb, lwb, w2, acc, e1, e1r, mb, mr,
    a_send, a_recv, f_send, f_recv, o_send, o_recv, z_send, z_recv, x_send, x_recv,
    p_send, p_recv, c_send, c_recv, y_send, y_recv,
):
    me = lax.axis_index("seq")
    row = lax.axis_index("row")
    other = 1 - row
    chip, core = me // 2, lax.rem(me, 2)
    mate = 2 * chip + (1 - core)
    rows = q_ref.shape[0]
    half = lw_ref.shape[0] // 2

    def at(number):
        return lax.rem(number + 2 * chips, chips)

    def heads_of(number):
        return pl.ds(pl.multiple_of(number * HEAD, HEAD), HEAD)

    ow_copy = pltpu.make_async_copy(ow_hbm, ow_ref, ow_sem)
    ow_copy.start()
    shard = hi_ref.shape[0]
    wb[me, :shard] = hi_ref[...]
    wb[me, shard:] = ho_ref[...]
    greet([(2 * at(chip + d) + core, row) for d in range(1, chips)] + [(mate, row), (me, other)])

    own = heads_of(chip)
    sends = []
    arrivals = {}
    own_half = pl.ds(pl.multiple_of(core * half, half), half)
    mate_half = pl.ds(pl.multiple_of((1 - core) * half, half), half)
    lw_copy = remote(lw_ref.at[own_half], lwb.at[own_half], y_send.at[0], y_recv.at[0], me, other)
    lw_copy.start()
    forwards = {}
    order = sorted(range(1, chips), key=lambda d: -min(d, chips - d))
    for d in order:
        to = at(chip + d)
        for which, (src, dst) in enumerate(
            ((k_ref, kb.at[me]), (v_ref, vb.at[me]), (q_ref, qb.at[chip]))
        ):
            copy = remote(
                src.at[:, heads_of(to)], dst, a_send.at[which, d], a_recv.at[which, d],
                2 * to + core, row,
            )
            copy.start()
            arrivals[which, d] = copy
    for which, (src, dst) in enumerate(((k_ref, kb), (v_ref, vb))):
        copy = remote(
            src.at[:, own], dst.at[me], f_send.at[which, 0], f_recv.at[which, 0], mate, row
        )
        copy.start()
        forwards[which, 0] = copy
    cot_copy = remote(cot_ref, cotb, c_send.at[0], c_recv.at[0], me, other)
    cot_copy.start()

    levels = chips // depth
    level, side = chip // depth, lax.rem(chip, depth)
    z_copies = []
    for d in range(1, levels):
        to = lax.rem(level + d, levels) * depth + side
        copy = remote(wb.at[me], wb.at[me], z_send.at[d], z_recv.at[d], 2 * to + core, row)
        copy.start()
        z_copies.append((d, copy))
    neighbour = 2 * (level * depth + (1 - side)) + core
    x_copies = []
    p_copies = []

    def pass_side(d, src, slot):
        copy = remote(src, wb.at[slot], x_send.at[d], x_recv.at[d], neighbour, row)
        copy.start()
        x_copies.append((d, copy))

    def pass_mate(number, src, slot):
        copy = remote(src, wb.at[slot], p_send.at[number], p_recv.at[number], mate, row)
        copy.start()
        p_copies.append(copy)

    pass_side(0, wb.at[me], me)
    pass_mate(0, wb.at[me], me)

    qb[chip] = q_ref[:, own]
    kb[me] = k_ref[:, own]
    vb[me] = v_ref[:, own]

    mb[...] = jnp.dot(
        gu_ref[...], lw_ref[...], preferred_element_type=jnp.float32
    ).astype(jnp.bfloat16)
    m_copy = remote(mb, mr, y_send.at[2], y_recv.at[2], me, other)
    m_copy.start()

    width = lw_ref.shape[0]
    tile = math.gcd(ow_ref.shape[0], 256)
    columns = lw_ref.shape[1]

    ow_copy.wait()

    @pl.loop(0, ow_ref.shape[0] // tile)
    def _(index):
        part = pl.ds(pl.multiple_of(index * tile, tile), tile)
        acc[part] = jnp.dot(
            ow_ref[part, pl.ds(pl.multiple_of(row * width, width), width)],
            lw_ref[...],
            preferred_element_type=jnp.float32,
        )

    lw_copy.wait_recv()
    lw_mate = remote(lwb.at[own_half], lwb.at[own_half], y_send.at[1], y_recv.at[1], mate, row)
    lw_mate.start()
    lw_mate.wait_recv()

    @pl.loop(0, ow_ref.shape[0] // tile)
    def _(index):
        part = pl.ds(pl.multiple_of(index * tile, tile), tile)
        total = acc[part] + jnp.dot(
            ow_ref[part, pl.ds(pl.multiple_of(other * width, width), width)],
            lwb[...],
            preferred_element_type=jnp.float32,
        )
        w2[part] = total.astype(jnp.bfloat16)

    for d in reversed(range(1, chips)):
        for which, buffer in ((0, kb), (1, vb)):
            arrivals[which, d].wait_recv()
            slot = 2 * at(chip - d) + core
            copy = remote(
                buffer.at[slot], buffer.at[slot], f_send.at[which, d], f_recv.at[which, d],
                mate, row,
            )
            copy.start()
            forwards[which, d] = copy
        arrivals[2, d].wait_recv()
    for copy in forwards.values():
        copy.wait_recv()

    scale = 1.0 / math.sqrt(HEAD)
    for i in reversed(range(chips)):
        span = (2 * i + 2) * rows
        keys = kb[: 2 * i + 2].reshape(span, HEAD)
        values = vb[: 2 * i + 2].reshape(span, HEAD)
        scores = contract(qb[i], keys, 1, 1) * scale
        last = 2 * rows
        places = lax.broadcasted_iota(jnp.int32, (rows, span), 1)
        queries = lax.broadcasted_iota(jnp.int32, (rows, span), 0) + (2 * i + core) * rows
        scores = jnp.where(places <= queries, scores, -1e30)
        top = jnp.max(scores, axis=1, keepdims=True)
        weights = jnp.exp(scores - top)
        mass = jnp.sum(weights, axis=1, keepdims=True)
        mixed = jnp.dot(weights.astype(jnp.bfloat16), values, preferred_element_type=jnp.float32)
        ob[i] = (mixed / mass).astype(jnp.bfloat16)

        @pl.when(i != chip)
        def _():
            remote(
                ob.at[i], att.at[:, own], o_send.at[i], o_recv.at[chip], 2 * i + core, row
            ).start()

        @pl.when(i == chip)
        def _():
            att[:, own] = ob[i]

    for d, copy in z_copies:
        copy.wait_recv()
        slot = 2 * (lax.rem(level - d + levels, levels) * depth + side) + core
        pass_side(d, wb.at[slot], slot)
        pass_mate(d, wb.at[slot], slot)
    for d, copy in list(x_copies):
        copy.wait_recv()
        slot = 2 * (lax.rem(level - d + levels, levels) * depth + (1 - side)) + core
        pass_mate(levels + d, wb.at[slot], slot)

    for i in range(chips):

        @pl.when(i != chip)
        def _():
            back = remote(
                ob.at[i], att.at[:, heads_of(i)], o_send.at[i], o_recv.at[i], 2 * i + core, row
            )
            back.wait_recv()
            back.wait_send()

    value = jnp.dot(att[...], w2[...], preferred_element_type=jnp.float32)
    e1[:, :columns] = (
        value
        + jnp.dot(res_ref[...], lw_ref[...], preferred_element_type=jnp.float32)
    ).astype(jnp.bfloat16)
    e1[:, columns:] = jnp.zeros((rows, e1.shape[1] - columns), jnp.bfloat16)
    e1[:, columns : columns + gd_ref.shape[0]] = contract(att[...], gd_ref[...], 1, 1).astype(
        jnp.bfloat16
    )
    e_copy = remote(e1, e1r, y_send.at[3], y_recv.at[3], me, other)
    e_copy.start()
    att_out[...] = att[...]
    cot_copy.wait_recv()
    cot_out[row] = cot_ref[...]
    cot_out[other] = cotb[...]
    m_copy.wait_recv()
    m_out[...] = mb[...].astype(jnp.float32) + mr[...].astype(jnp.float32)
    for copy in p_copies:
        copy.wait_recv()
    hi_out[...] = wb[:, :shard]
    ho_out[...] = wb[:, shard:]
    e_copy.wait_recv()
    proj_out[...] = e1[...].astype(jnp.float32) + e1r[...].astype(jnp.float32)
    for copy in (
        [lw_copy, lw_mate, cot_copy, m_copy, e_copy]
        + list(arrivals.values())
        + list(forwards.values())
        + [copy for d, copy in z_copies + x_copies]
        + p_copies
    ):
        copy.wait_send()


def front(q, k, v, hi, ho, cot, ow, lw, gd, gu, res, count):
    chips = q.shape[1] // HEAD
    rows = q.shape[0]
    depth = 2
    levels = chips // depth
    columns = lw.shape[1]
    wide = columns + HEAD
    vm = pl.BlockSpec(memory_space=pltpu.VMEM)
    dma = pltpu.SemaphoreType.DMA
    bf, f32 = jnp.bfloat16, jnp.float32
    return pl.pallas_call(
        functools.partial(front_kernel, chips, depth),
        out_shape=(
            jax.ShapeDtypeStruct(q.shape, bf),
            jax.ShapeDtypeStruct((rows, wide), f32),
            jax.ShapeDtypeStruct((gu.shape[0], columns), f32),
            jax.ShapeDtypeStruct((count,) + hi.shape, bf),
            jax.ShapeDtypeStruct((count,) + ho.shape, bf),
            jax.ShapeDtypeStruct((2,) + cot.shape, bf),
        ),
        in_specs=[vm] * 6 + [pl.BlockSpec(memory_space=pl.ANY)] + [vm] * 4,
        out_specs=(vm,) * 6,
        scratch_shapes=[
            pltpu.VMEM(ow.shape, bf),
            dma,
            pltpu.VMEM((chips, rows, HEAD), bf),
            pltpu.VMEM((count, rows, HEAD), bf),
            pltpu.VMEM((count, rows, HEAD), bf),
            pltpu.VMEM((chips, rows, HEAD), bf),
            pltpu.VMEM(q.shape, bf),
            pltpu.VMEM((count, 2 * hi.shape[0], hi.shape[1]), bf),
            pltpu.VMEM(cot.shape, bf),
            pltpu.VMEM(lw.shape, bf),
            pltpu.VMEM((ow.shape[0], columns), bf),
            pltpu.VMEM((ow.shape[0], columns), f32),
            pltpu.VMEM((rows, wide), bf),
            pltpu.VMEM((rows, wide), bf),
            pltpu.VMEM((gu.shape[0], columns), bf),
            pltpu.VMEM((gu.shape[0], columns), bf),
            dma((3, chips)), dma((3, chips)),
            dma((2, chips)), dma((2, chips)),
            dma((chips,)), dma((chips,)),
            dma((levels,)), dma((levels,)),
            dma((levels,)), dma((levels,)),
            dma((chips,)), dma((chips,)),
            dma((1,)), dma((1,)),
            dma((4,)), dma((4,)),
        ],
        compiler_params=pltpu.CompilerParams(
            collective_id=0, has_side_effects=True, vmem_limit_bytes=60 * 1024 * 1024
        ),
        name="front",
    )(q, k, v, hi, ho, cot, ow, lw, gd, gu, res)


def swap_kernel(x_ref, o_ref, buf, send, recv):
    me, row = lax.axis_index("seq"), lax.axis_index("row")
    greet([(me, 1 - row)])
    copy = remote(x_ref, buf, send, recv, me, 1 - row)
    copy.start()
    copy.wait()
    o_ref[...] = x_ref[...].astype(jnp.float32) + buf[...].astype(jnp.float32)


def row_sum(x):
    vm = pl.BlockSpec(memory_space=pltpu.VMEM)
    return pl.pallas_call(
        swap_kernel,
        out_shape=jax.ShapeDtypeStruct(x.shape, jnp.float32),
        in_specs=[vm],
        out_specs=vm,
        scratch_shapes=[
            pltpu.VMEM(x.shape, x.dtype), pltpu.SemaphoreType.DMA, pltpu.SemaphoreType.DMA
        ],
        compiler_params=pltpu.CompilerParams(collective_id=1, has_side_effects=True),
        name="row_sum",
    )(x)


def total_kernel(count, shared, g_ref, o_ref, part, result, full, s1, r1, s2, r2, s3, r3):
    me, row = lax.axis_index("seq"), lax.axis_index("row")
    other = 1 - row
    peers = [(lax.rem(me + d, count), row) for d in range(1, count)]
    cross = [(lax.rem(me + d, count), other) for d in range(count)]
    greet(peers + cross)
    first = []
    for d in range(1, count):
        to = lax.rem(me + d, count)
        copy = remote(g_ref.at[to], part.at[row, me], s1.at[d], r1.at[d], to, row)
        copy.start()
        first.append(copy)
    crossing = []
    for index, to in enumerate(shared):
        copy = remote(g_ref.at[to], part.at[row, me], s3.at[index], r3.at[me], to, other)
        copy.start()
        crossing.append(copy)
    part[row, me] = g_ref[me]
    for copy in first:
        copy.wait_recv()

    def add(side):
        return jnp.sum(part[side].astype(jnp.float32), axis=0)

    result[...] = add(row).astype(jnp.bfloat16)

    @pl.when(me >= shared[0])
    def _():
        for source in range(count):
            remote(
                g_ref.at[0], part.at[other, source], s3.at[0], r3.at[source], me, other
            ).wait_recv()
        result[...] = (add(0) + add(1)).astype(jnp.bfloat16)

    second = []
    for d in range(1, count):
        to = lax.rem(me + d, count)
        copy = remote(result, full.at[me], s2.at[d], r2.at[d], to, row)
        copy.start()
        second.append(copy)
    full[me] = result[...]
    for copy in second:
        copy.wait_recv()
    o_ref[...] = full[...].astype(jnp.float32)
    for copy in first + crossing + second:
        copy.wait_send()


def grand_total(g, shared):
    count = g.shape[0]
    vm = pl.BlockSpec(memory_space=pltpu.VMEM)
    dma = pltpu.SemaphoreType.DMA
    return pl.pallas_call(
        functools.partial(total_kernel, count, shared),
        out_shape=jax.ShapeDtypeStruct(g.shape, jnp.float32),
        in_specs=[vm],
        out_specs=vm,
        scratch_shapes=[
            pltpu.VMEM((2,) + g.shape, g.dtype),
            pltpu.VMEM(g.shape[1:], g.dtype),
            pltpu.VMEM(g.shape, g.dtype),
            dma((count,)), dma((count,)),
            dma((count,)), dma((count,)),
            dma((len(shared),)), dma((count,)),
        ],
        compiler_params=pltpu.CompilerParams(collective_id=2, has_side_effects=True),
        name="grand_total",
    )(g)


def paired_body(
    patch_queries,
    patch_keys,
    patch_values,
    patch_tasks,
    residual,
    output_weight,
    global_down,
    global_up,
    global_scales,
    local_weight,
    byte_ids,
    byte_table,
    position_table,
    norm_gain,
    hidden_in,
    hidden_out,
    local_down,
    local_up,
    local_scales,
    cotangent,
):
    count = lax.axis_size("seq")
    bf = jnp.bfloat16
    rank = global_up.shape[0]
    columns = local_weight.shape[1]
    hidden = hidden_in.shape[0]
    attended, proj, bridge, rows_in, rows_out, cot = front(
        patch_queries, patch_keys, patch_values, jnp.transpose(hidden_in),
        jnp.transpose(hidden_out), cotangent, output_weight, local_weight,
        jnp.transpose(global_down), global_up, residual, count,
    )
    reduced = proj[:, columns : columns + rank]
    rows_in = rows_in.reshape(columns, hidden)
    rows_out = rows_out.reshape(columns, hidden)
    cot = cot.reshape(-1, columns)
    task_scales = select_rows(global_scales, patch_tasks)
    scaled = (reduced * task_scales).astype(bf)
    bridge_b = bridge.astype(bf)
    projected = (
        proj[:, :columns] + jnp.dot(scaled, bridge_b, preferred_element_type=jnp.float32)
    ).astype(bf)
    inputs, inverse, normed, lowered, scales, shrunk, byte_tasks = local_inputs(
        byte_ids, projected, patch_tasks, byte_table, position_table, norm_gain, local_down,
        local_scales,
    )
    upper = jnp.dot(normed, rows_in, preferred_element_type=jnp.float32) + jnp.dot(
        shrunk, local_up, preferred_element_type=jnp.float32
    )
    through = jnp.dot(cot, rows_out, preferred_element_type=jnp.float32)
    grown = (through * gelu_slope(upper)).astype(bf)
    grad_local_up = contract(shrunk, grown, 0, 0)
    back_rank = contract(grown, local_up, 1, 1)
    moved = (back_rank * scales).astype(bf)
    grad_local_scales = task_totals(byte_tasks, back_rank * lowered)
    grad_local_down = contract(moved, normed, 0, 0)
    back_total = contract(grown, rows_in, 1, 1) + contract(moved, local_down, 1, 1)
    gained = back_total * norm_gain
    average = jnp.mean(gained * inputs, axis=1, keepdims=True)
    back_inputs = inverse * (gained - inputs * inverse * inverse * average)
    patches = patch_tasks.shape[0]
    back_part = back_inputs.reshape(patches, PATCH, -1).sum(axis=1).astype(bf)
    cot_sum = cot.astype(jnp.float32).reshape(patches, PATCH, -1).sum(axis=1)
    patch_grad = (row_sum(back_part) + cot_sum).astype(bf)
    back_mixed = contract(patch_grad, local_weight, 1, 1).astype(bf)
    grad_global_up = contract(scaled, back_mixed, 0, 0)
    back_scaled = contract(patch_grad, bridge_b, 1, 1)
    grad_global_scales = task_totals(patch_tasks, back_scaled * reduced)
    back_reduced = (back_scaled * task_scales).astype(bf)
    grad_global_down = contract(back_reduced, attended, 0, 0)

    spare = hidden - columns - rank
    small = jnp.concatenate([0.5 * grad_global_scales, grad_local_scales], axis=0)
    last = jnp.concatenate(
        [grad_local_down, small, jnp.zeros((rank, spare), jnp.float32)], axis=1
    )
    packed = jnp.concatenate(
        [grad_global_down, grad_global_up, grad_local_up, last], axis=0
    ).astype(bf)
    blocks = packed.reshape(count, 16, -1)
    shared = tuple(range(count - count // 4, count))
    summed = grand_total(blocks, shared).reshape(packed.shape)
    last = summed[3 * rank :]
    return (
        jnp.transpose(summed[:rank]),
        summed[rank : 2 * rank],
        last[:TASKS, columns : columns + rank],
        jnp.transpose(last[:, :columns]),
        summed[2 * rank : 3 * rank],
        last[TASKS:, columns : columns + rank],
    )


def pick_body(seq_count, row_count, *args):
    heads = args[0].shape[1] // HEAD
    rank = args[7].shape[0]
    hidden = args[14].shape[0]
    fits = (
        row_count == 2
        and seq_count == 2 * heads
        and heads % 4 == 0
        and rank == 2 * TASKS
        and args[0].shape[1] == hidden
        and (4 * rank * hidden) % (seq_count * 16 * HEAD) == 0
        and hidden >= args[9].shape[1] + rank
    )
    return paired_body(*args) if fits else general_body(*args)


def solution(mesh):
    placed = (
        P("seq", "row"),
        P("seq", "row"),
        P("seq", "row"),
        P("seq"),
        P("seq", "row"),
        P("row", None),
        P("row", None),
        P(None, "row"),
        P(),
        P("row", None),
        P("seq"),
        P(),
        P(),
        P(),
        P("row", "seq"),
        P("row", "seq"),
        P(),
        P(None, "row"),
        P(),
        P(("seq", "row"), None),
    )
    chosen = functools.partial(pick_body, mesh.shape["seq"], mesh.shape["row"])
    return jax.shard_map(
        chosen,
        mesh=mesh,
        in_specs=placed,
        out_specs=(P("row", None), P(None, "row"), P(), P(), P(None, "row"), P()),
        check_vma=False,
    )
```
